32 devices in a mesh: parts: 2 (over y), seq: 4 (over z), tok: 2 (over x), head: 2 (over core).
Axes of the slice: x: 2, y: 2, z: 4, core: 2. Of those that a mesh axis runs over, the one named last changes fastest.
Arguments:
- values: bfloat16 [8192, 2048], P(('parts', 'seq', 'tok'), 'head'), parts along dimension 0, may hold values from -6 to 6
- key_rows: bfloat16 [8192, 128], P(('parts', 'seq', 'tok')), parts along dimension 0, may hold values from -0.5 to 0.5
- query_rows: bfloat16 [8192, 128], P(('parts', 'seq', 'tok')), parts along dimension 0, may hold values from -6 to 6
- decay_codes: int32 [32, 8192], P('head', ('parts', 'seq', 'tok')), parts along dimension 1, may hold values from 0 to 48398, as said below
- weight_codes: int32 [12, 32, 8192], P(None, 'head', ('parts', 'seq', 'tok')), parts along dimension 2, may hold values from 16 to 511
- norm_gain: float32 [2048], P('head'), may hold values from 0.5 to 1.5
Outputs:
- mixed: bfloat16 [8192, 2048], P(('parts', 'seq', 'tok'), 'head'), parts along dimension 0
The draws below stay inside these ranges and needn't reach their ends.
There are 2 independent parts, one for each index of `parts`. The reference program is written for one: setup_inputs(seed, part) draws one part's arguments, and reference() takes and returns one part's arrays. A program takes and returns all parts, laid end to end along the dimension named above; an argument that names none is the same for every part. Nothing has to cross between parts.
Inputs may be any that keep to these rules, and one draw needn't show every extreme that they name: `decay_codes`: Log-decay numerators over 65536. `weight_codes`: level weight numerators over 256.
All inputs are finite; a program needn't handle non-finite values.
Results may differ from the reference program's by a relative error of at most 0.0048.
Values sent between devices are 32-bit elements; how exact they have to be, the bound alone decides.
No kernel may reach another device: no remote copies, remote signals or barrier semaphores. Data moves between devices by JAX's collectives and lax.ppermute only.
A program may use at most 64 MiB of HBM per device.

```python
import jax
import jax.numpy as jnp
from jax import lax

HEAD_TOTAL = 32
P_SIZE = 64
N = 128
BUCKET = 64
LEVELS = 12
TOK_DEV = 512
TOKEN_TOTAL = 4096
N_SEQ = 4
N_TOK = 2


def draw_decay_codes(key, part):
    random_seed_key = jax.random.fold_in(key, 7)
    selector_random_key, gradual_random_key, quick_random_key, position_random_key, spike_random_key = jax.random.split(random_seed_key, 5)
    quick_head_flags = jax.random.randint(selector_random_key, (HEAD_TOTAL, 1), 0, 2)
    gradual_decay_labels = jax.random.randint(gradual_random_key, (HEAD_TOTAL, TOKEN_TOTAL), 0, 1 + 131072 // TOKEN_TOTAL)
    quick_decay_labels = jax.random.randint(quick_random_key, (HEAD_TOTAL, TOKEN_TOTAL), 1000, 3000)
    spike_positions = jax.random.randint(position_random_key, (4,), 0, TOKEN_TOTAL)
    spike_position = jnp.any(jnp.arange(TOKEN_TOTAL)[:, None] == spike_positions[None, :], axis=1)
    spike_decay_labels = jax.random.randint(spike_random_key, (HEAD_TOTAL, TOKEN_TOTAL), 14600, 45400)
    return jnp.where(quick_head_flags == 1, quick_decay_labels, gradual_decay_labels) + jnp.where(spike_position[None, :], spike_decay_labels, 0)


def plant(entries, own_key, least, largest):
    spot = [jax.random.randint(jax.random.fold_in(own_key, axis), (), 0, length) for axis, length in enumerate(entries.shape)]
    main_axis = entries.shape.index(max(entries.shape))
    beside = spot[:main_axis] + [(spot[main_axis] + 1) % entries.shape[main_axis]] + spot[main_axis + 1:]
    return entries.at[tuple(spot)].set(least).at[tuple(beside)].set(largest)


def shard_levels(own_key, extent, cuts, low, top_value):
    gain = 1.0
    for position, parts in cuts:
        heights = jax.random.uniform(jax.random.fold_in(jax.random.fold_in(own_key, 6), position), (parts,), jnp.float32, low / len(cuts), top_value / len(cuts))
        gain = gain * jnp.repeat(jnp.exp(heights), extent[position] // parts).reshape((-1,) + (1,) * (len(extent) - 1 - position))
    return gain


def noise(rng, dims, scale, bound, cuts=(), held_as=jnp.bfloat16):
    values = scale * jax.random.normal(rng, dims, jnp.float32)
    if cuts:
        values = values * shard_levels(rng, dims, cuts, -0.22, 0.18)
    return jnp.clip(values, -bound, bound).astype(held_as)


def setup_inputs(seed: int = 0, part: int = 0) -> dict:
    streams_of = jax.random.split(jax.random.key(seed), 7)
    part_keys = jax.random.split(jax.random.fold_in(streams_of[6], part), 7)
    return {
        "values": noise(part_keys[0], (TOKEN_TOTAL, HEAD_TOTAL * P_SIZE), 1.0, 6.0, ((0, 8), (1, 2))),
        "key_rows": noise(part_keys[1], (TOKEN_TOTAL, N), N ** -0.5, 0.5, ((0, 8),)),
        "query_rows": noise(part_keys[2], (TOKEN_TOTAL, N), 1.0, 6.0, ((0, 8),)),
        "decay_codes": draw_decay_codes(jax.random.fold_in(jax.random.fold_in(streams_of[6], part), 71), part),
        "weight_codes": plant(jax.random.randint(part_keys[4], (LEVELS, HEAD_TOTAL, TOKEN_TOTAL), 16, 512), jax.random.fold_in(part_keys[4], 1), 16, 511).astype(jnp.int32),
        "norm_gain": jnp.clip(1.0 + 0.1 * jax.random.normal(streams_of[5], (HEAD_TOTAL * P_SIZE,), jnp.float32), 0.5, 1.5),
    }


decay_denominator = 65536.0
weight_denominator = 256.0
norm_epsilon = 1e-05
row_limit = 512
highest = lax.Precision.HIGHEST

def bit_count(numbers, width_bits):
    result = jnp.zeros(numbers.shape, jnp.int32)
    for bit_place in range(width_bits):
        result = result + (numbers >= 1 << bit_place).astype(jnp.int32)
    return result

def token_spread(levels_full, lam_rows, slot_count):
    spread = jnp.zeros(levels_full.shape, jnp.float32)
    for slot in range(slot_count):
        spread = spread + jnp.where(levels_full == slot, lam_rows[slot][:, None], 0.0)
    return spread

def decay_sums(decay_codes):
    return jnp.cumsum(-decay_codes.astype(jnp.float32) / decay_denominator, axis=1)

def near_terms(values, key_rows, query_rows, cumulative, level_scale, head_size):
    token_count = values.shape[0]
    head_count = cumulative.shape[0]
    buckets = token_count // BUCKET
    level_bits = (buckets - 1).bit_length()
    bucket_ids = jnp.arange(buckets, dtype=jnp.int32)
    levels = bit_count(jnp.bitwise_xor(bucket_ids[:, None], bucket_ids[None, :]), level_bits)
    head_weights = jnp.transpose(level_scale[:level_bits + 1], (1, 0, 2))
    block_rows = min(row_limit, token_count)
    pieces = []
    for row_start in range(0, token_count, block_rows):
        row_end = row_start + block_rows
        scores = jnp.einsum('tn,sn->ts', query_rows[row_start:row_end], key_rows[:row_end], preferred_element_type=jnp.float32)
        causal = jnp.arange(row_start, row_end)[:, None] >= jnp.arange(row_end)[None, :]
        tiles = levels[row_start // BUCKET:row_end // BUCKET, :row_end // BUCKET]
        levels_full = jnp.broadcast_to(tiles[:, None, :, None], (block_rows // BUCKET, BUCKET, row_end // BUCKET, BUCKET)).reshape(block_rows, row_end)

        def one_head(head_item):
            cum_rates, weights, head_index = head_item
            log_gap = jnp.where(causal, cum_rates[row_start:row_end, None] - cum_rates[None, :row_end], 0.0)
            spread = token_spread(levels_full, weights[:, row_start:row_end], level_bits + 1)
            mixing = jnp.where(causal, jnp.exp(log_gap) * spread * scores, 0.0).astype(jnp.bfloat16)
            columns = lax.dynamic_slice_in_dim(values[:row_end], head_index * head_size, head_size, 1)
            return jnp.dot(mixing, columns, preferred_element_type=jnp.float32)
        pieces.append(lax.map(one_head, (cumulative, head_weights, jnp.arange(head_count, dtype=jnp.int32))))
    return jnp.concatenate(pieces, axis=1)

def block_state(values, key_rows, cumulative, head_size):
    token_count = values.shape[0]
    head_count = cumulative.shape[0]
    end_decay = jnp.exp(cumulative[:, -1:] - cumulative)
    decayed = (values.astype(jnp.float32).reshape(token_count, head_count, head_size) * end_decay.T[:, :, None]).astype(jnp.bfloat16)
    return jnp.einsum('tn,thp->hnp', key_rows, decayed, preferred_element_type=jnp.float32)

def decay_coeff(sources, own_index, log_gap):
    earlier = (sources < own_index)[:, None]
    return jnp.where(earlier, jnp.exp(jnp.where(earlier, log_gap, 0.0)), 0.0)

def level_onehot(levels, slot_ids):
    return (levels[:, None] == slot_ids[None, :]).astype(jnp.float32)

def finish(near, far_levels, far_weights, query_rows, cumulative, norm_gain, head_size):
    token_count = query_rows.shape[0]
    head_count = cumulative.shape[0]
    queries = query_rows.astype(jnp.float32)
    readout = jnp.zeros(near.shape, jnp.float32)
    for slot in range(far_levels.shape[0]):
        part_out = jnp.einsum('tn,hnp->htp', queries, far_levels[slot], precision=highest)
        readout = readout + far_weights[slot][:, :, None] * part_out
    combined = near + jnp.exp(cumulative)[:, :, None] * readout
    inverse_rms = lax.rsqrt(lax.optimization_barrier(jnp.mean(combined * combined, axis=2, keepdims=True)) + norm_epsilon)
    normed = combined * inverse_rms * norm_gain.astype(jnp.float32).reshape(head_count, 1, head_size)
    return jnp.transpose(normed, (1, 0, 2)).reshape(token_count, head_count * head_size).astype(jnp.bfloat16)

def reference(values, key_rows, query_rows, decay_codes, weight_codes, norm_gain):
    devices = N_SEQ * N_TOK
    value_blocks = values.reshape(devices, TOK_DEV, HEAD_TOTAL * P_SIZE)
    key_blocks = key_rows.reshape(devices, TOK_DEV, N)
    query_blocks = query_rows.reshape(devices, TOK_DEV, N)
    code_blocks = jnp.transpose(decay_codes.reshape(HEAD_TOTAL, devices, TOK_DEV), (1, 0, 2))
    weight_blocks = jnp.transpose(weight_codes.reshape(LEVELS, HEAD_TOTAL, devices, TOK_DEV), (2, 0, 1, 3))

    def state_of(block_item):
        block_values, block_keys, block_codes = block_item
        cumulative = decay_sums(block_codes)
        return (block_state(block_values, block_keys, cumulative, P_SIZE), cumulative[:, -1])
    states, totals = lax.map(state_of, (value_blocks, key_blocks, code_blocks))
    inclusive = jnp.cumsum(totals, axis=0)
    exclusive = inclusive - totals
    base_level = (TOK_DEV // BUCKET).bit_length() - 1
    device_bits = (devices - 1).bit_length()
    sources = jnp.arange(devices, dtype=jnp.int32)
    slot_ids = base_level + 1 + jnp.arange(device_bits, dtype=jnp.int32)

    def output_of(block_item):
        block_index, block_values, block_keys, block_queries, block_codes, block_weights = block_item
        cumulative = decay_sums(block_codes)
        level_scale = block_weights.astype(jnp.float32) / weight_denominator
        near = near_terms(block_values, block_keys, block_queries, cumulative, level_scale, P_SIZE)
        log_gap = exclusive[block_index][None, :] - inclusive
        coefficient = decay_coeff(sources, block_index, log_gap)
        levels = base_level + bit_count(jnp.bitwise_xor(sources, block_index), device_bits)
        onehot = level_onehot(levels, slot_ids)
        far_levels = jnp.einsum('mh,mj,mhnp->jhnp', coefficient, onehot, states, precision=highest)
        far_weights = level_scale[base_level + 1:base_level + 1 + device_bits]
        return finish(near, far_levels, far_weights, block_queries, cumulative, norm_gain, P_SIZE)
    outputs = lax.map(output_of, (sources, value_blocks, key_blocks, query_blocks, code_blocks, weight_blocks))
    return outputs.reshape(TOKEN_TOTAL, HEAD_TOTAL * P_SIZE)
```

```python
import functools

import jax
import jax.numpy as jnp
from jax import lax
from jax.experimental import pallas as pl
from jax.experimental.pallas import tpu as pltpu
from jax.sharding import PartitionSpec as P

BUCKET = 64
LANES = 128
CHUNKS = 4

decay_unit = 1.0 / 65536.0
weight_unit = 1.0 / 256.0
norm_epsilon = 1e-05
masked_out = -1e30

bf16 = jnp.bfloat16
f32 = jnp.float32


def contract_last(a, b):
    return lax.dot_general(a, b, (((1,), (1,)), ((), ())), preferred_element_type=f32)


def split_two(x):
    high = x.astype(bf16)
    return high, (x - high.astype(f32)).astype(bf16)


def decay_exponents(codes):
    heads, tokens = codes.shape
    blocks = tokens // LANES
    high = (codes >> 8).astype(f32).astype(bf16)
    low = (codes & 255).astype(f32).astype(bf16)
    stacked = jnp.concatenate(
        [part[:, LANES * j : LANES * (j + 1)] for j in range(blocks) for part in (high, low)], axis=0
    )
    row = lax.broadcasted_iota(jnp.int32, (LANES, LANES), 0)
    col = lax.broadcasted_iota(jnp.int32, (LANES, LANES), 1)
    same = (row // BUCKET) == (col // BUCKET)
    upto = row <= col

    def sums(mask):
        weights = jnp.where(mask, 1.0, 0.0).astype(bf16)
        out = jnp.dot(stacked, weights, preferred_element_type=f32)
        return [
            out[2 * heads * j : 2 * heads * j + heads] * 256.0
            + out[2 * heads * j + heads : 2 * heads * (j + 1)]
            for j in range(blocks)
        ]

    prefix = {BUCKET: sums(same & upto), LANES: sums(upto)}
    suffix = {BUCKET: sums(same & ~upto), LANES: sums(~upto)}
    total = sums(row >= 0)
    size = 2 * LANES
    while size <= tokens:
        span = size // LANES
        prefix[size], suffix[size] = [], []
        for j in range(blocks):
            start = j // span * span
            prefix[size].append(sum(total[start:j], prefix[LANES][j]))
            suffix[size].append(sum(total[j + 1 : start + span], suffix[LANES][j]))
        size *= 2
    everything = sum(total[1:], total[0])
    join = lambda pieces: jnp.concatenate(pieces, axis=1)
    return (
        {k: join(v) for k, v in prefix.items()},
        {k: join(v) for k, v in suffix.items()},
        everything,
    )


def state_kernel(rows, values_ref, keys_ref, codes_ref, weights_ref, *outs):
    payloads, turned_ref, source_ref, reader_ref, cum_ref = outs[:-4], *outs[-4:]
    heads, tokens = codes_ref.shape
    head_size = values_ref.shape[1] // heads
    prefix, suffix, total = decay_exponents(codes_ref[...])
    cum_ref[...] = prefix[tokens] * -decay_unit
    sizes = [BUCKET]
    while sizes[-1] * 2 < tokens:
        sizes.append(sizes[-1] * 2)
    for i, size in enumerate(sizes):
        source_ref[i] = jnp.exp(suffix[size] * -decay_unit)
    lam = lambda level: weights_ref[level].astype(f32) * weight_unit
    reader_ref[0] = lam(0) * jnp.exp(suffix[BUCKET] * decay_unit)
    for i, size in enumerate(sizes):
        reader_ref[i + 1] = lam(i + 1) * jnp.exp(prefix[size] * -decay_unit)
    to_end = jnp.exp(suffix[tokens] * -decay_unit)
    total = total * -decay_unit
    keys = keys_ref[...]
    chunk_heads = rows // head_size
    for c, payload in enumerate(payloads):
        turned = values_ref[:, rows * c : rows * (c + 1)].T
        turned_ref[rows * c : rows * (c + 1), :] = turned
        decayed = jnp.concatenate(
            [
                (
                    turned[head_size * i : head_size * (i + 1)].astype(f32)
                    * to_end[chunk_heads * c + i : chunk_heads * c + i + 1]
                ).astype(bf16)
                for i in range(chunk_heads)
            ],
            axis=0,
        )
        payload[:rows, :] = jnp.dot(decayed, keys, preferred_element_type=f32)
        payload[rows : rows + chunk_heads, :] = total[chunk_heads * c : chunk_heads * (c + 1)]
        pad = payload.shape[0] - rows - chunk_heads
        if pad:
            payload[rows + chunk_heads :, :] = jnp.zeros((pad, LANES), f32)


def near_kernel(chunk_heads, turned_ref, queries_ref, keys_ref, source_ref, reader_ref, *refs):
    outs, table_ref = refs[:-1], refs[-1]
    tokens = queries_ref.shape[0]
    heads = source_ref.shape[1]
    rows = outs[0].shape[0]
    head_size = rows // chunk_heads
    blocks = tokens // LANES
    row = lax.broadcasted_iota(jnp.int32, (LANES, LANES), 0)
    col = lax.broadcasted_iota(jnp.int32, (LANES, LANES), 1)
    same = (row // BUCKET) == (col // BUCKET)
    for j in range(blocks):
        span = pl.ds(LANES * j, LANES)
        scores = contract_last(keys_ref[span, :], queries_ref[span, :])
        inner = jnp.where(same & (row <= col), scores, 0.0)
        across = jnp.where(~same & (row < col), scores, 0.0)
        table_ref[j] = jnp.concatenate(split_two(jnp.concatenate([inner, across], axis=1)), axis=0)
    wide = {}
    size = LANES
    while size < tokens:
        wide[size] = []
        for start in range(0, tokens, 2 * size):
            scores = contract_last(
                keys_ref[pl.ds(start, size), :], queries_ref[pl.ds(start + size, size), :]
            )
            wide[size].append(jnp.concatenate(split_two(scores), axis=0))
        size *= 2

    def scaled(c, level, low, high):
        pieces = []
        for i in range(chunk_heads):
            part = turned_ref[pl.ds(rows * c + head_size * i, head_size), low:high].astype(f32)
            factor = source_ref[level, chunk_heads * c + i : chunk_heads * c + i + 1, low:high]
            pieces.append((part * factor).astype(bf16))
        piece = jnp.concatenate(pieces, axis=0)
        return jnp.concatenate([piece, piece], axis=1)

    def read(c, level, low, high, product):
        pieces = []
        for i in range(chunk_heads):
            factor = reader_ref[level, chunk_heads * c + i : chunk_heads * c + i + 1, low:high]
            pieces.append(product[head_size * i : head_size * (i + 1)] * factor)
        return jnp.concatenate(pieces, axis=0)

    for c, out in enumerate(outs):
        for j in range(blocks):
            low, high = LANES * j, LANES * (j + 1)
            product = jnp.dot(scaled(c, 0, low, high), table_ref[j], preferred_element_type=f32)
            out[:, low:high] = read(c, 0, low, high, product[:, :LANES]) + read(
                c, 1, low, high, product[:, LANES:]
            )
        level = 2
        for size, tables in wide.items():
            for g, table in enumerate(tables):
                start = 2 * size * g
                product = jnp.dot(
                    scaled(c, level - 1, start, start + size), table, preferred_element_type=f32
                )
                low, high = start + size, start + 2 * size
                out[:, low:high] = out[:, low:high] + read(c, level, low, high, product)
            level += 1


def finish_kernel(chunk, chunk_heads, base_level, far_count, *refs):
    near_ref, queries_ref, cum_ref, weights_ref, gain_ref = refs[:5]
    far_refs, gap_refs = refs[5 : 5 + far_count], refs[5 + far_count : 5 + 2 * far_count]
    out_ref = refs[-1]
    rows, tokens = near_ref.shape
    head_size = rows // chunk_heads
    first = chunk_heads * chunk
    cum = cum_ref[first : first + chunk_heads, :]
    queries = queries_ref[...]
    doubled = jnp.concatenate([queries, queries], axis=1)
    combined = [near_ref[head_size * i : head_size * (i + 1), :] for i in range(chunk_heads)]
    for slot in range(far_count):
        product = contract_last(jnp.concatenate(split_two(far_refs[slot][...]), axis=1), doubled)
        gap = jnp.concatenate([gap_refs[slot][...]] * (tokens // LANES), axis=1)
        lam = weights_ref[base_level + 1 + slot, first : first + chunk_heads, :].astype(f32)
        factor = lam * weight_unit * jnp.exp(cum + gap)
        for i in range(chunk_heads):
            combined[i] = combined[i] + factor[i : i + 1] * product[head_size * i : head_size * (i + 1)]
    gain = jnp.broadcast_to(gain_ref[0:1, rows * chunk : rows * (chunk + 1)], (LANES, rows)).T
    pieces = []
    for i in range(chunk_heads):
        y = combined[i]
        inverse = lax.rsqrt(jnp.sum(y * y, axis=0, keepdims=True) * (1.0 / head_size) + norm_epsilon)
        own_gain = jnp.concatenate(
            [gain[head_size * i : head_size * (i + 1)]] * (tokens // LANES), axis=1
        )
        pieces.append((y * inverse * own_gain).astype(bf16))
    out_ref[...] = jnp.concatenate(pieces, axis=0).T


vmem = functools.partial(pl.BlockSpec, memory_space=pltpu.VMEM)
params = pltpu.CompilerParams(vmem_limit_bytes=56 * 1024 * 1024)


def local(values, key_rows, query_rows, decay_codes, weight_codes, norm_gain):
    heads, tokens = decay_codes.shape
    columns = values.shape[1]
    head_size = columns // heads
    chunks = CHUNKS
    rows = columns // chunks
    chunk_heads = heads // chunks
    state_size = key_rows.shape[1]
    near_levels = (tokens // BUCKET).bit_length()
    padded = rows + -(-chunk_heads // 8) * 8
    tok_count, seq_count = lax.axis_size("tok"), lax.axis_size("seq")
    tok_bits, seq_bits = tok_count.bit_length() - 1, seq_count.bit_length() - 1
    tok_index = lax.axis_index("tok")

    *payloads, turned, source, reader, cum = pl.pallas_call(
        functools.partial(state_kernel, rows),
        name="state",
        out_shape=[jax.ShapeDtypeStruct((padded, state_size), f32)] * chunks
        + [
            jax.ShapeDtypeStruct((columns, tokens), bf16),
            jax.ShapeDtypeStruct((near_levels - 1, heads, tokens), f32),
            jax.ShapeDtypeStruct((near_levels, heads, tokens), f32),
            jax.ShapeDtypeStruct((heads, tokens), f32),
        ],
        in_specs=[vmem()] * 4,
        out_specs=[vmem()] * (chunks + 4),
        compiler_params=params,
    )(values, key_rows, decay_codes, weight_codes)

    near = pl.pallas_call(
        functools.partial(near_kernel, chunk_heads),
        name="near",
        out_shape=[jax.ShapeDtypeStruct((rows, tokens), f32)] * chunks,
        in_specs=[vmem()] * 5,
        out_specs=[vmem()] * chunks,
        scratch_shapes=[pltpu.VMEM((tokens // LANES, 2 * LANES, 2 * LANES), bf16)],
        compiler_params=params,
    )(turned, query_rows, key_rows, source, reader)

    def spread(per_head):
        return jnp.broadcast_to(
            per_head[:, None, :], (chunk_heads, head_size, state_size)
        ).reshape(rows, state_size)

    finished = []
    for c in range(chunks):
        aggregate = payloads[c][:rows]
        total = payloads[c][rows : rows + chunk_heads]
        payload = payloads[c]
        prefix = jnp.zeros_like(total)
        far, gaps = [], []
        for place in range(tok_bits):
            if place:
                payload = jnp.concatenate(
                    [aggregate, total, jnp.zeros((padded - rows - chunk_heads, state_size), f32)]
                )
            pairs = [(i, i ^ (1 << place)) for i in range(tok_count)]
            received = lax.ppermute(payload, "tok", pairs)
            partner, partner_total = received[:rows], received[rows : rows + chunk_heads]
            upper = (tok_index >> place) & 1 == 1
            far.append(partner)
            gaps.append(jnp.where(upper, prefix, masked_out))
            decay = jnp.exp(jnp.where(upper, total, partner_total))
            aggregate = jnp.where(
                upper, spread(decay) * partner + aggregate, spread(decay) * aggregate + partner
            )
            prefix = jnp.where(upper, prefix + partner_total, prefix)
            total = total + partner_total
        group_decay = jnp.exp(total)
        for place in range(seq_bits):
            half = 1 << place
            carried = lax.ppermute(
                aggregate, "seq", [(b + half - 1, b + half) for b in range(0, seq_count, 2 * half)]
            )
            for step in range(1, half):
                carried = carried + lax.ppermute(
                    spread(group_decay) * carried,
                    "seq",
                    [(b + half + step - 1, b + half + step) for b in range(0, seq_count, 2 * half)],
                )
            far.append(carried)
            gaps.append(prefix)
            if place + 1 < seq_bits:
                aggregate = aggregate + spread(group_decay) * carried
        finished.append((far, gaps))

    far_count = tok_bits + seq_bits
    gain = norm_gain.reshape(1, columns)
    out = None
    for c, (far, gaps) in enumerate(finished):
        operands = [near[c], query_rows, cum, weight_codes, gain, *far, *gaps]
        in_specs = [vmem()] * len(operands)
        aliases = {}
        if out is not None:
            aliases = {len(operands): 0}
            operands.append(out)
            in_specs.append(pl.BlockSpec(memory_space=pl.ANY))
        out = pl.pallas_call(
            functools.partial(finish_kernel, c, chunk_heads, near_levels - 1, far_count),
            name=f"finish{c}",
            grid=(1,),
            out_shape=jax.ShapeDtypeStruct((tokens, columns), bf16),
            in_specs=in_specs,
            out_specs=pl.BlockSpec((tokens, rows), lambda i, c=c: (0, c)),
            input_output_aliases=aliases,
            compiler_params=params,
        )(*operands)
    return out


def solution(mesh):
    return jax.shard_map(
        local,
        mesh=mesh,
        in_specs=(
            P(("parts", "seq", "tok"), "head"),
            P(("parts", "seq", "tok"), None),
            P(("parts", "seq", "tok"), None),
            P("head", ("parts", "seq", "tok")),
            P(None, "head", ("parts", "seq", "tok")),
            P("head"),
        ),
        out_specs=P(("parts", "seq", "tok"), "head"),
        check_vma=False,
    )
```

```python
import functools

import jax
import jax.numpy as jnp
from jax import lax
from jax.experimental import pallas as pl
from jax.experimental.pallas import tpu as pltpu
from jax.sharding import PartitionSpec as P


BUCKET = 64
LANES = 128
PIECES = 2

decay_unit = 1.0 / 65536.0
weight_unit = 1.0 / 256.0
norm_epsilon = 1e-05
masked_out = -1e30

bf16 = jnp.bfloat16
f32 = jnp.float32


def contract_last(a, b):
    return lax.dot_general(a, b, (((1,), (1,)), ((), ())), preferred_element_type=f32)


def split_two(x):
    high = x.astype(bf16)
    return high, (x - high.astype(f32)).astype(bf16)


def decay_exponents(codes):
    heads, tokens = codes.shape
    blocks = tokens // LANES
    high = (codes >> 8).astype(f32).astype(bf16)
    low = (codes & 255).astype(f32).astype(bf16)
    stacked = jnp.concatenate(
        [part[:, LANES * j : LANES * (j + 1)] for j in range(blocks) for part in (high, low)], axis=0
    )
    row = lax.broadcasted_iota(jnp.int32, (LANES, LANES), 0)
    col = lax.broadcasted_iota(jnp.int32, (LANES, LANES), 1)
    same = (row // BUCKET) == (col // BUCKET)
    upto = row <= col

    def sums(mask):
        weights = jnp.where(mask, 1.0, 0.0).astype(bf16)
        out = jnp.dot(stacked, weights, preferred_element_type=f32)
        return [
            out[2 * heads * j : 2 * heads * j + heads] * 256.0
            + out[2 * heads * j + heads : 2 * heads * (j + 1)]
            for j in range(blocks)
        ]

    prefix = {BUCKET: sums(same & upto), LANES: sums(upto)}
    suffix = {BUCKET: sums(same & ~upto), LANES: sums(~upto)}
    total = sums(row >= 0)
    size = 2 * LANES
    while size <= tokens:
        span = size // LANES
        prefix[size], suffix[size] = [], []
        for j in range(blocks):
            start = j // span * span
            prefix[size].append(sum(total[start:j], prefix[LANES][j]))
            suffix[size].append(sum(total[j + 1 : start + span], suffix[LANES][j]))
        size *= 2
    everything = sum(total[1:], total[0])
    join = lambda pieces: jnp.concatenate(pieces, axis=1)
    return (
        {k: join(v) for k, v in prefix.items()},
        {k: join(v) for k, v in suffix.items()},
        everything,
    )


def half_order(swap):
    own = lax.axis_index("tok") if swap else 0
    return (own, 1 - own)


def start_halves(source, target, sems, dim, swap):
    extent = source.shape[dim] // 2
    copies = []
    for place, half in enumerate(half_order(swap)):
        take = [pl.ds(0, n) for n in source.shape]
        put = list(take)
        start = half * extent
        take[dim] = pl.ds(start if isinstance(start, int) else pl.multiple_of(start, extent), extent)
        put[dim] = pl.ds(place * extent, extent)
        copy = pltpu.make_async_copy(source.at[tuple(take)], target.at[tuple(put)], sems.at[place])
        copy.start()
        copies.append(copy)
    return copies


def state_kernel(pieces, order, swap, with_totals, values_hbm, keys_hbm, queries_hbm, codes_hbm, *refs):
    count = len(pieces)
    states = refs[:count]
    total_ref, turned_ref, source_ref, reader_ref, cum_ref, keys_ref, queries_ref = refs[count : count + 7]
    values_ref, codes_ref, value_sems, code_sems, row_sems = refs[count + 7 :]
    code_copies = start_halves(codes_hbm, codes_ref, code_sems, 0, swap)
    value_copies = start_halves(values_hbm, values_ref, value_sems, 1, swap)
    key_copy = pltpu.make_async_copy(keys_hbm, keys_ref, row_sems.at[0])
    key_copy.start()
    query_copy = pltpu.make_async_copy(queries_hbm, queries_ref, row_sems.at[1])
    query_copy.start()
    for copy in code_copies:
        copy.wait()
    heads, tokens = codes_ref.shape
    head_size = values_ref.shape[1] // heads
    prefix, suffix, total = decay_exponents(codes_ref[...])
    cum_ref[...] = prefix[tokens] * -decay_unit
    sizes = [BUCKET]
    while sizes[-1] * 2 < tokens:
        sizes.append(sizes[-1] * 2)
    for i, size in enumerate(sizes):
        source_ref[i] = jnp.exp(suffix[size] * -decay_unit)
    reader_ref[0] = jnp.exp(suffix[BUCKET] * decay_unit)
    for i, size in enumerate(sizes):
        reader_ref[i + 1] = jnp.exp(prefix[size] * -decay_unit)
    to_end = jnp.exp(suffix[tokens] * -decay_unit)
    total = total * -decay_unit
    total_ref[...] = total
    key_copy.wait()
    for copy in value_copies:
        copy.wait()
    keys = keys_ref[...]
    for c in order:
        first, size = pieces[c]
        low, rows = first * head_size, size * head_size
        turned = values_ref[:, low : low + rows].T
        turned_ref[low : low + rows, :] = turned
        decayed = jnp.concatenate(
            [
                (
                    turned[head_size * i : head_size * (i + 1)].astype(f32) * to_end[first + i : first + i + 1]
                ).astype(bf16)
                for i in range(size)
            ],
            axis=0,
        )
        states[c][:rows, :] = jnp.dot(decayed, keys, preferred_element_type=f32)
        if c == with_totals:
            states[c][rows:, :] = total
    query_copy.wait()


def near_kernel(
    pieces, swap, turned_ref, queries_ref, keys_ref, source_ref, decay_ref, cum_ref, weights_hbm, gain_hbm, *refs
):
    count = len(pieces)
    outs_hbm, far_ref, gain_ref = refs[:count], refs[count], refs[count + 1]
    table_ref, reader_ref, weights_ref, weight_sems, gain_sems = refs[count + 2 : count + 7]
    outs, out_sems = refs[count + 7 : -1], refs[-1]
    copies = start_halves(weights_hbm, weights_ref, weight_sems, 1, swap)
    copies += start_halves(gain_hbm, gain_ref, gain_sems, 1, swap)
    tokens = queries_ref.shape[0]
    near_levels, heads, _ = decay_ref.shape
    head_size = turned_ref.shape[0] // heads
    blocks = tokens // LANES
    row = lax.broadcasted_iota(jnp.int32, (LANES, LANES), 0)
    col = lax.broadcasted_iota(jnp.int32, (LANES, LANES), 1)
    same = (row // BUCKET) == (col // BUCKET)
    for j in range(blocks):
        span = pl.ds(LANES * j, LANES)
        scores = contract_last(keys_ref[span, :], queries_ref[span, :])
        inner = jnp.where(same & (row <= col), scores, 0.0)
        across = jnp.where(~same & (row < col), scores, 0.0)
        table_ref[j] = jnp.concatenate(split_two(jnp.concatenate([inner, across], axis=1)), axis=0)
    wide = {}
    size = LANES
    while size < tokens:
        wide[size] = []
        for start in range(0, tokens, 2 * size):
            scores = contract_last(
                keys_ref[pl.ds(start, size), :], queries_ref[pl.ds(start + size, size), :]
            )
            wide[size].append(jnp.concatenate(split_two(scores), axis=0))
        size *= 2
    for copy in copies:
        copy.wait()
    for level in range(near_levels):
        reader_ref[level] = weights_ref[level].astype(f32) * weight_unit * decay_ref[level]
    own_decay = jnp.exp(cum_ref[...])
    for slot in range(far_ref.shape[0]):
        far_ref[slot] = weights_ref[near_levels + slot].astype(f32) * weight_unit * own_decay

    stores = []
    for c, ((first, size), out) in enumerate(zip(pieces, outs)):

        def scaled(level, low, high):
            parts = []
            for h in range(first, first + size):
                part = turned_ref[pl.ds(head_size * h, head_size), low:high].astype(f32)
                parts.append((part * source_ref[level, h : h + 1, low:high]).astype(bf16))
            piece = jnp.concatenate(parts, axis=0)
            return jnp.concatenate([piece, piece], axis=1)

        def read(level, low, high, product):
            return jnp.concatenate(
                [
                    product[head_size * i : head_size * (i + 1)]
                    * reader_ref[level, first + i : first + i + 1, low:high]
                    for i in range(size)
                ],
                axis=0,
            )

        for j in range(blocks):
            low, high = LANES * j, LANES * (j + 1)
            product = jnp.dot(scaled(0, low, high), table_ref[j], preferred_element_type=f32)
            out[:, low:high] = read(0, low, high, product[:, :LANES]) + read(
                1, low, high, product[:, LANES:]
            )
        level = 2
        for span, tables in wide.items():
            for g, table in enumerate(tables):
                start = 2 * span * g
                product = jnp.dot(scaled(level - 1, start, start + span), table, preferred_element_type=f32)
                low, high = start + span, start + 2 * span
                out[:, low:high] = out[:, low:high] + read(level, low, high, product)
            level += 1
        store = pltpu.make_async_copy(out, outs_hbm[c], out_sems.at[c])
        store.start()
        stores.append(store)
    for store in stores:
        store.wait()


def finish_kernel(piece, swap, far_count, *refs):
    first, size = piece
    near_hbm, queries_ref, factor_ref, gain_ref = refs[:4]
    far_refs, gap_refs = refs[4 : 4 + far_count], refs[4 + far_count : 4 + 2 * far_count]
    out_hbm, out_ref, near_ref, sems = refs[-4:]
    load = pltpu.make_async_copy(near_hbm, near_ref, sems.at[0])
    load.start()
    rows, tokens = near_ref.shape
    heads = factor_ref.shape[1]
    head_size = rows // size
    queries = queries_ref[...]
    doubled = jnp.concatenate([queries, queries], axis=1)
    combined = [0.0] * size
    for slot in range(far_count):
        product = contract_last(jnp.concatenate(split_two(far_refs[slot][:rows, :]), axis=1), doubled)
        gap = jnp.exp(gap_refs[slot][first : first + size, :])
        factor = factor_ref[slot, first : first + size, :] * jnp.concatenate([gap] * (tokens // LANES), axis=1)
        for i in range(size):
            combined[i] = combined[i] + factor[i : i + 1] * product[head_size * i : head_size * (i + 1)]
    low = first * head_size
    gain = jnp.broadcast_to(gain_ref[0:1, low : low + rows], (LANES, rows)).T
    load.wait()
    parts = []
    for i in range(size):
        y = combined[i] + near_ref[head_size * i : head_size * (i + 1), :]
        inverse = lax.rsqrt(jnp.sum(y * y, axis=0, keepdims=True) * (1.0 / head_size) + norm_epsilon)
        own_gain = jnp.concatenate([gain[head_size * i : head_size * (i + 1)]] * (tokens // LANES), axis=1)
        parts.append((y * inverse * own_gain).astype(bf16))
    out_ref[...] = jnp.concatenate(parts, axis=0).T
    half = heads // 2
    column = half_order(swap)[first // half] * (half * head_size) + (first % half) * head_size
    if not isinstance(column, int):
        column = pl.multiple_of(column, LANES)
    store = pltpu.make_async_copy(out_ref, out_hbm.at[:, pl.ds(column, rows)], sems.at[1])
    store.start()
    store.wait()


vmem = functools.partial(pl.BlockSpec, memory_space=pltpu.VMEM)
hbm = functools.partial(pl.BlockSpec, memory_space=pltpu.HBM)
params = pltpu.CompilerParams(vmem_limit_bytes=16 * 1024 * 1024)
dma = pltpu.SemaphoreType.DMA


def in_hbm(x):
    return pltpu.with_memory_space_constraint(x, pltpu.HBM)


def spread(per_head, head_size):
    size, lanes = per_head.shape
    return jnp.broadcast_to(per_head[:, None, :], (size, head_size, lanes)).reshape(size * head_size, lanes)


def both_ways(bases, low):
    return [pair for b in bases for pair in ((b + low, b + low + 1), (b + low + 1, b + low))]


def one_way(bases, low):
    return [(b + low, b + low + 1) for b in bases]


def exchange_all(states, total, pieces, head_size):
    tok_count, seq_count = lax.axis_size("tok"), lax.axis_size("seq")
    tok_bits, seq_bits = tok_count.bit_length() - 1, seq_count.bit_length() - 1
    tok_index = lax.axis_index("tok")
    own_total, gaps = total, []
    prefix = jnp.zeros_like(total)
    aggregates, far = list(states), [[] for _ in states]
    for place in range(tok_bits):
        pairs = [(i, i ^ (1 << place)) for i in range(tok_count)]
        upper = (tok_index >> place) & 1 == 1
        partner_total = lax.ppermute(own_total, "tok", pairs)
        decay = jnp.exp(jnp.where(upper, own_total, partner_total))
        for c, (first, size) in enumerate(pieces):
            partner = lax.ppermute(aggregates[c], "tok", pairs)
            factor = spread(decay[first : first + size], head_size)
            far[c].append(partner)
            aggregates[c] = jnp.where(upper, factor * partner + aggregates[c], factor * aggregates[c] + partner)
        gaps.append(jnp.where(upper, prefix, masked_out))
        prefix = jnp.where(upper, prefix + partner_total, prefix)
        own_total = own_total + partner_total
    decay = jnp.exp(own_total)
    for place in range(seq_bits):
        half = 1 << place
        bases = range(0, seq_count, 2 * half)
        for c, (first, size) in enumerate(pieces):
            factor = spread(decay[first : first + size], head_size)
            carried = lax.ppermute(aggregates[c], "seq", [(b + half - 1, b + half) for b in bases])
            for step in range(1, half):
                carried = carried + lax.ppermute(
                    factor * carried, "seq", [(b + half + step - 1, b + half + step) for b in bases]
                )
            far[c].append(carried)
            aggregates[c] = aggregates[c] + factor * carried
        gaps.append(prefix)
    return far, gaps


def exchange_halves(states, total, pieces, head_size):
    seq_count = lax.axis_size("seq")
    seq_bits = seq_count.bit_length() - 1
    upper = lax.axis_index("tok") == 1
    seq_index = lax.axis_index("seq")
    swap = [(0, 1), (1, 0)]
    count = len(pieces) // 2
    heads = total.shape[0]
    half_heads = heads // 2
    far = [[] for _ in pieces]
    aggregates = []
    for i in range(count):
        first, size = pieces[i]
        rows = size * head_size
        received = lax.ppermute(states[count + i], "tok", swap)
        if i == 0:
            partner_total = received[rows:]
            partner_total = jnp.concatenate([partner_total[half_heads:], partner_total[:half_heads]])
            decay = jnp.exp(jnp.where(upper, total, partner_total))
        partner, own = received[:rows], states[i]
        factor = spread(decay[first : first + size], head_size)
        far[i].append(partner)
        aggregates.append(jnp.where(upper, factor * partner + own, factor * own + partner))
    for i in range(count):
        far[count + i].append(lax.ppermute(states[i], "tok", swap))
    prefix = jnp.where(upper, partner_total, 0.0)
    gaps = [jnp.where(upper, jnp.zeros_like(total), masked_out)]
    group_decay = jnp.exp(total + partner_total)
    for place in range(seq_bits):
        half = 1 << place
        bases = range(0, seq_count, 2 * half)
        for i in range(count):
            first, size = pieces[i]
            factor = spread(group_decay[first : first + size], head_size)
            first_hop = both_ways(bases, 0) if place == 0 else one_way(bases, half - 1)
            carried = lax.ppermute(aggregates[i], "seq", first_hop)
            for step in range(1, half):
                arrived = lax.ppermute(factor * carried, "seq", one_way(bases, half + step - 1))
                carried = jnp.where(seq_index % (2 * half) == half + step, arrived, carried)
            far[i].append(carried)
            far[count + i].append(lax.ppermute(carried, "tok", swap))
            aggregates[i] = aggregates[i] + factor * carried
        gaps.append(jnp.where((seq_index >> place) & 1 == 1, prefix, masked_out))
    return far, gaps


def local(values, key_rows, query_rows, decay_codes, weight_codes, norm_gain):
    heads, tokens = decay_codes.shape
    columns = values.shape[1]
    head_size = columns // heads
    state_size = key_rows.shape[1]
    near_levels = (tokens // BUCKET).bit_length()
    far_count = lax.axis_size("tok").bit_length() + lax.axis_size("seq").bit_length() - 2
    swap = lax.axis_size("tok") == 2
    half = heads // 2
    count = PIECES
    size = half // count
    pieces = [(size * i, size) for i in range(2 * count)]
    order = [*range(count, 2 * count), *range(count)]
    with_totals = count if swap else None

    *states, total, turned, source, decay, cum, keys, queries = pl.pallas_call(
        functools.partial(state_kernel, pieces, order, swap, with_totals),
        name="state",
        out_shape=[
            jax.ShapeDtypeStruct((n * head_size + (heads if c == with_totals else 0), state_size), f32)
            for c, (_, n) in enumerate(pieces)
        ]
        + [
            jax.ShapeDtypeStruct((heads, LANES), f32),
            jax.ShapeDtypeStruct((columns, tokens), bf16),
            jax.ShapeDtypeStruct((near_levels - 1, heads, tokens), f32),
            jax.ShapeDtypeStruct((near_levels, heads, tokens), f32),
            jax.ShapeDtypeStruct((heads, tokens), f32),
            jax.ShapeDtypeStruct(key_rows.shape, key_rows.dtype),
            jax.ShapeDtypeStruct(query_rows.shape, query_rows.dtype),
        ],
        in_specs=[hbm()] * 4,
        out_specs=[vmem()] * (len(pieces) + 7),
        scratch_shapes=[
            pltpu.VMEM(values.shape, values.dtype),
            pltpu.VMEM(decay_codes.shape, decay_codes.dtype),
            dma((2,)),
            dma((2,)),
            dma((2,)),
        ],
        compiler_params=params,
    )(*(in_hbm(x) for x in (values, key_rows, query_rows, decay_codes)))

    near_call = pl.pallas_call(
        functools.partial(near_kernel, pieces, swap),
        name="near",
        out_shape=[pltpu.HBM((n * head_size, tokens), f32) for _, n in pieces]
        + [
            jax.ShapeDtypeStruct((far_count, heads, tokens), f32),
            jax.ShapeDtypeStruct((1, columns), f32),
        ],
        in_specs=[vmem()] * 6 + [hbm()] * 2,
        out_specs=[hbm()] * len(pieces) + [vmem()] * 2,
        scratch_shapes=[
            pltpu.VMEM((tokens // LANES, 2 * LANES, 2 * LANES), bf16),
            pltpu.VMEM((near_levels, heads, tokens), f32),
            pltpu.VMEM(weight_codes.shape, weight_codes.dtype),
            dma((2,)),
            dma((2,)),
        ]
        + [pltpu.VMEM((n * head_size, tokens), f32) for _, n in pieces]
        + [dma((len(pieces),))],
        compiler_params=params,
    )
    *near, far_factor, gain = near_call(
        turned, queries, keys, source, decay, cum, in_hbm(weight_codes), in_hbm(norm_gain.reshape(1, columns))
    )

    exchange = exchange_halves if swap else exchange_all
    far, gaps = exchange(states, total, pieces, head_size)
    out = None
    for c, piece in enumerate(pieces):
        rows = piece[1] * head_size
        operands = [near[c], queries, far_factor, gain, *far[c], *gaps]
        in_specs = [hbm()] + [vmem()] * (len(operands) - 1)
        aliases = {}
        if out is not None:
            aliases = {len(operands): 0}
            operands.append(out)
            in_specs.append(hbm())
        finish_call = pl.pallas_call(
            functools.partial(finish_kernel, piece, swap, far_count),
            out_shape=pltpu.HBM((tokens, columns), bf16),
            in_specs=in_specs,
            out_specs=hbm(),
            scratch_shapes=[pltpu.VMEM((tokens, rows), bf16), pltpu.VMEM((rows, tokens), f32), dma((2,))],
            input_output_aliases=aliases,
            compiler_params=params,
        )
        out = finish_call(*operands)
    return out


def solution(mesh):
    return jax.shard_map(
        local,
        mesh=mesh,
        in_specs=(
            P(("parts", "seq", "tok"), "head"),
            P(("parts", "seq", "tok"), None),
            P(("parts", "seq", "tok"), None),
            P("head", ("parts", "seq", "tok")),
            P(None, "head", ("parts", "seq", "tok")),
            P("head"),
        ),
        out_specs=P(("parts", "seq", "tok"), "head"),
        check_vma=False,
    )
```

```python
import functools

import jax
import jax.numpy as jnp
from jax import lax
from jax.experimental import pallas as pl
from jax.experimental.pallas import tpu as pltpu
from jax.sharding import PartitionSpec as P


BUCKET = 64
LANES = 128
PIECE_SHARES = (1, 1)

decay_unit = 1.0 / 65536.0
weight_unit = 1.0 / 256.0
norm_epsilon = 1e-05
masked_out = -1e30

bf16 = jnp.bfloat16
f32 = jnp.float32


def contract_last(a, b):
    return lax.dot_general(a, b, (((1,), (1,)), ((), ())), preferred_element_type=f32)


def split_two(x):
    high = x.astype(bf16)
    return high, (x - high.astype(f32)).astype(bf16)


def decay_exponents(codes):
    heads, tokens = codes.shape
    blocks = tokens // LANES
    high = (codes >> 8).astype(f32).astype(bf16)
    low = (codes & 255).astype(f32).astype(bf16)
    stacked = jnp.concatenate(
        [part[:, LANES * j : LANES * (j + 1)] for j in range(blocks) for part in (high, low)], axis=0
    )
    row = lax.broadcasted_iota(jnp.int32, (LANES, LANES), 0)
    col = lax.broadcasted_iota(jnp.int32, (LANES, LANES), 1)
    same = (row // BUCKET) == (col // BUCKET)
    upto = row <= col

    def sums(mask):
        weights = jnp.where(mask, 1.0, 0.0).astype(bf16)
        out = jnp.dot(stacked, weights, preferred_element_type=f32)
        return [
            out[2 * heads * j : 2 * heads * j + heads] * 256.0
            + out[2 * heads * j + heads : 2 * heads * (j + 1)]
            for j in range(blocks)
        ]

    prefix = {BUCKET: sums(same & upto), LANES: sums(upto)}
    suffix = {BUCKET: sums(same & ~upto), LANES: sums(~upto)}
    total = sums(row >= 0)
    size = 2 * LANES
    while size <= tokens:
        span = size // LANES
        prefix[size], suffix[size] = [], []
        for j in range(blocks):
            start = j // span * span
            prefix[size].append(sum(total[start:j], prefix[LANES][j]))
            suffix[size].append(sum(total[j + 1 : start + span], suffix[LANES][j]))
        size *= 2
    everything = sum(total[1:], total[0])
    join = lambda pieces: jnp.concatenate(pieces, axis=1)
    return (
        {k: join(v) for k, v in prefix.items()},
        {k: join(v) for k, v in suffix.items()},
        everything,
    )


def half_order(swap):
    own = lax.axis_index("tok") if swap else 0
    return (own, 1 - own)


def start_half(source, target, sem, dim, half):
    extent = source.shape[dim] // 2
    take = [pl.ds(0, n) for n in source.shape]
    start = half * extent
    take[dim] = pl.ds(start if isinstance(start, int) else pl.multiple_of(start, extent), extent)
    copy = pltpu.make_async_copy(source.at[tuple(take)], target, sem)
    copy.start()
    return copy


def start_halves(source, target, sems, dim, swap):
    extent = source.shape[dim] // 2
    copies = []
    for place, half in enumerate(half_order(swap)):
        put = [pl.ds(0, n) for n in source.shape]
        put[dim] = pl.ds(place * extent, extent)
        copies.append(start_half(source, target.at[tuple(put)], sems.at[place], dim, half))
    return copies


def decayed_state(turned, to_end, keys, first, size, base):
    head_size = turned.shape[0] // (to_end.shape[0] // 2)
    parts = []
    for h in range(first, first + size):
        row = (h - base) * head_size
        parts.append((turned[row : row + head_size].astype(f32) * to_end[h : h + 1]).astype(bf16))
    return jnp.dot(jnp.concatenate(parts, axis=0), keys, preferred_element_type=f32)


def state_kernel(pieces, swap, values_hbm, keys_hbm, queries_hbm, codes_hbm, *refs):
    count = len(pieces) // 2
    states = refs[:count]
    total_ref, turned_ref, source_ref, reader_ref, cum_ref, end_ref, keys_ref, queries_ref = refs[count : count + 8]
    values_ref, codes_ref, code_sems, row_sems = refs[count + 8 :]
    code_copies = start_halves(codes_hbm, codes_ref, code_sems, 0, swap)
    key_copy = pltpu.make_async_copy(keys_hbm, keys_ref, row_sems.at[0])
    key_copy.start()
    value_copy = start_half(values_hbm, values_ref, row_sems.at[1], 1, half_order(swap)[1])
    query_copy = pltpu.make_async_copy(queries_hbm, queries_ref, row_sems.at[2])
    query_copy.start()
    for copy in code_copies:
        copy.wait()
    heads, tokens = codes_ref.shape
    prefix, suffix, total = decay_exponents(codes_ref[...])
    cum_ref[...] = prefix[tokens] * -decay_unit
    sizes = [BUCKET]
    while sizes[-1] * 2 < tokens:
        sizes.append(sizes[-1] * 2)
    for i, size in enumerate(sizes):
        source_ref[i] = jnp.exp(suffix[size] * -decay_unit)
    reader_ref[0] = jnp.exp(suffix[BUCKET] * decay_unit)
    for i, size in enumerate(sizes):
        reader_ref[i + 1] = jnp.exp(prefix[size] * -decay_unit)
    to_end = jnp.exp(suffix[tokens] * -decay_unit)
    end_ref[...] = to_end
    total = total * -decay_unit
    total_ref[...] = total
    key_copy.wait()
    value_copy.wait()
    keys = keys_ref[...]
    head_size = 2 * values_ref.shape[1] // heads
    base = pieces[count][0]
    for state_ref, (first, size) in zip(states, pieces[count:]):
        low, rows = (first - base) * head_size, size * head_size
        turned_ref[low : low + rows, :] = values_ref[:, low : low + rows].T
        state_ref[:rows, :] = decayed_state(turned_ref, to_end, keys, first, size, base)
        if state_ref.shape[0] > rows:
            state_ref[rows:, :] = total
    query_copy.wait()


def near_kernel(
    pieces,
    swap,
    own_splits,
    other_ref,
    queries_ref,
    keys_ref,
    source_ref,
    decay_ref,
    cum_ref,
    end_ref,
    weights_hbm,
    gain_hbm,
    values_hbm,
    *refs,
):
    count = len(pieces)
    outs_hbm, far_ref, gain_ref = refs[:count], refs[count], refs[count + 1]
    state_refs, refs = refs[count + 2 : count + 2 + own_splits], refs[count + 2 + own_splits :]
    table_ref, reader_ref, weights_ref, values_ref, own_ref, weight_sems, gain_sems, value_sem = refs[:8]
    outs, out_sems = refs[8:-1], refs[-1]
    value_copy = start_half(values_hbm, values_ref, value_sem, 1, half_order(swap)[0])
    copies = start_halves(weights_hbm, weights_ref, weight_sems, 1, swap)
    copies += start_halves(gain_hbm, gain_ref, gain_sems, 1, swap)
    tokens = queries_ref.shape[0]
    near_levels, heads, _ = decay_ref.shape
    head_size = 2 * other_ref.shape[0] // heads
    blocks = tokens // LANES
    row = lax.broadcasted_iota(jnp.int32, (LANES, LANES), 0)
    col = lax.broadcasted_iota(jnp.int32, (LANES, LANES), 1)
    same = (row // BUCKET) == (col // BUCKET)
    for j in range(blocks):
        span = pl.ds(LANES * j, LANES)
        scores = contract_last(keys_ref[span, :], queries_ref[span, :])
        inner = jnp.where(same & (row <= col), scores, 0.0)
        across = jnp.where(~same & (row < col), scores, 0.0)
        table_ref[j] = jnp.concatenate(split_two(jnp.concatenate([inner, across], axis=1)), axis=0)
    wide = {}
    size = LANES
    while size < tokens:
        wide[size] = []
        for start in range(0, tokens, 2 * size):
            scores = contract_last(
                keys_ref[pl.ds(start, size), :], queries_ref[pl.ds(start + size, size), :]
            )
            wide[size].append(jnp.concatenate(split_two(scores), axis=0))
        size *= 2
    for copy in copies:
        copy.wait()
    for level in range(near_levels):
        reader_ref[level] = weights_ref[level].astype(f32) * weight_unit * decay_ref[level]
    own_decay = jnp.exp(cum_ref[...])
    for slot in range(far_ref.shape[0]):
        far_ref[slot] = weights_ref[near_levels + slot].astype(f32) * weight_unit * own_decay

    value_copy.wait()
    own_ref[...] = values_ref[...].T
    row = 0
    for state_ref in state_refs:
        rows = state_ref.shape[0]
        state_ref[...] = decayed_state(
            own_ref, end_ref[...], keys_ref[...], row // head_size, rows // head_size, 0
        )
        row += rows
    stores = []
    for c, ((first, size), out) in enumerate(zip(pieces, outs)):

        def scaled(level, low, high):
            parts = []
            for h in range(first, first + size):
                turned_ref, place = (own_ref, h) if h < heads // 2 else (other_ref, h - heads // 2)
                part = turned_ref[pl.ds(head_size * place, head_size), low:high].astype(f32)
                parts.append((part * source_ref[level, h : h + 1, low:high]).astype(bf16))
            piece = jnp.concatenate(parts, axis=0)
            return jnp.concatenate([piece, piece], axis=1)

        def read(level, low, high, product):
            return jnp.concatenate(
                [
                    product[head_size * i : head_size * (i + 1)]
                    * reader_ref[level, first + i : first + i + 1, low:high]
                    for i in range(size)
                ],
                axis=0,
            )

        for j in range(blocks):
            low, high = LANES * j, LANES * (j + 1)
            product = jnp.dot(scaled(0, low, high), table_ref[j], preferred_element_type=f32)
            out[:, low:high] = read(0, low, high, product[:, :LANES]) + read(
                1, low, high, product[:, LANES:]
            )
        level = 2
        for span, tables in wide.items():
            for g, table in enumerate(tables):
                start = 2 * span * g
                product = jnp.dot(scaled(level - 1, start, start + span), table, preferred_element_type=f32)
                low, high = start + span, start + 2 * span
                out[:, low:high] = out[:, low:high] + read(level, low, high, product)
            level += 1
        store = pltpu.make_async_copy(out, outs_hbm[c], out_sems.at[c])
        store.start()
        stores.append(store)
    for store in stores:
        store.wait()


def finish_kernel(pieces, swap, far_count, far_rows, done_count, stores_all, *refs):
    first, size = pieces[-1]
    near_ref, queries_ref, factor_ref, gain_ref = refs[:4]
    far_refs, gap_refs = refs[4 : 4 + far_count], refs[4 + far_count : 4 + 2 * far_count]
    rows, tokens = near_ref.shape
    heads = factor_ref.shape[1]
    head_size = rows // size
    stores = []

    def store(piece, source, target, sem):
        half = heads // 2
        column = half_order(swap)[piece[0] // half] * (half * head_size) + (piece[0] % half) * head_size
        if not isinstance(column, int):
            column = pl.multiple_of(column, LANES)
        copy = pltpu.make_async_copy(source, target.at[:, pl.ds(column, piece[1] * head_size)], sem)
        copy.start()
        stores.append(copy)

    out_ref = refs[4 + 2 * far_count]
    if stores_all:
        done_refs = refs[4 + 2 * far_count : 4 + 2 * far_count + done_count]
        out_hbm, out_ref, sems = refs[-3:]
        for c, done in enumerate(done_refs):
            store(pieces[c], done, out_hbm, sems.at[c])
    queries = queries_ref[...]
    doubled = jnp.concatenate([queries, queries], axis=1)
    stacked = jnp.concatenate(
        [
            jnp.concatenate(split_two(far[row : row + rows, :]), axis=1)
            for far, row in zip(far_refs, far_rows)
        ],
        axis=0,
    )
    products = contract_last(stacked, doubled)
    low = first * head_size
    gain = jnp.broadcast_to(gain_ref[0:1, low : low + rows], (LANES, rows)).T
    factors = []
    for slot in range(far_count):
        gap = jnp.exp(gap_refs[slot][first : first + size, :])
        factors.append(
            factor_ref[slot, first : first + size, :] * jnp.concatenate([gap] * (tokens // LANES), axis=1)
        )
    parts = []
    for i in range(size):
        y = near_ref[head_size * i : head_size * (i + 1), :]
        for slot in range(far_count):
            start = rows * slot + head_size * i
            y = y + factors[slot][i : i + 1] * products[start : start + head_size]
        inverse = lax.rsqrt(jnp.sum(y * y, axis=0, keepdims=True) * (1.0 / head_size) + norm_epsilon)
        own_gain = jnp.concatenate([gain[head_size * i : head_size * (i + 1)]] * (tokens // LANES), axis=1)
        parts.append((y * inverse * own_gain).astype(bf16))
    out_ref[...] = jnp.concatenate(parts, axis=0).T
    if stores_all:
        store(pieces[-1], out_ref, out_hbm, sems.at[done_count])
    for copy in stores:
        copy.wait()


vmem = functools.partial(pl.BlockSpec, memory_space=pltpu.VMEM)
hbm = functools.partial(pl.BlockSpec, memory_space=pltpu.HBM)
params = pltpu.CompilerParams(vmem_limit_bytes=16 * 1024 * 1024)
dma = pltpu.SemaphoreType.DMA


def in_hbm(x):
    return pltpu.with_memory_space_constraint(x, pltpu.HBM)


def spread(per_head, head_size):
    size, lanes = per_head.shape
    return jnp.broadcast_to(per_head[:, None, :], (size, head_size, lanes)).reshape(size * head_size, lanes)


def both_ways(bases, low):
    return [pair for b in bases for pair in ((b + low, b + low + 1), (b + low + 1, b + low))]


def one_way(bases, low):
    return [(b + low, b + low + 1) for b in bases]


def apart(x):
    return lax.optimization_barrier(x)


def exchange_all(states, total, pieces, head_size):
    tok_count, seq_count = lax.axis_size("tok"), lax.axis_size("seq")
    tok_bits, seq_bits = tok_count.bit_length() - 1, seq_count.bit_length() - 1
    tok_index = lax.axis_index("tok")
    own_total, gaps = total, []
    prefix = jnp.zeros_like(total)
    aggregates, far = list(states), [[] for _ in states]
    for place in range(tok_bits):
        pairs = [(i, i ^ (1 << place)) for i in range(tok_count)]
        upper = (tok_index >> place) & 1 == 1
        partner_total = lax.ppermute(own_total, "tok", pairs)
        decay = jnp.exp(jnp.where(upper, own_total, partner_total))
        for c, (first, size) in enumerate(pieces):
            partner = lax.ppermute(aggregates[c], "tok", pairs)
            factor = spread(decay[first : first + size], head_size)
            far[c].append((partner, 0))
            aggregates[c] = jnp.where(upper, factor * partner + aggregates[c], factor * aggregates[c] + partner)
        gaps.append(jnp.where(upper, prefix, masked_out))
        prefix = jnp.where(upper, prefix + partner_total, prefix)
        own_total = own_total + partner_total
    decay = jnp.exp(own_total)
    for place in range(seq_bits):
        half = 1 << place
        bases = range(0, seq_count, 2 * half)
        for c, (first, size) in enumerate(pieces):
            factor = spread(decay[first : first + size], head_size)
            carried = lax.ppermute(aggregates[c], "seq", [(b + half - 1, b + half) for b in bases])
            for step in range(1, half):
                carried = carried + lax.ppermute(
                    factor * carried, "seq", [(b + half + step - 1, b + half + step) for b in bases]
                )
            far[c].append((carried, 0))
            aggregates[c] = aggregates[c] + factor * carried
        gaps.append(prefix)
    return far, gaps


def exchange_halves(states, total, pieces, head_size):
    own_states, *given = states
    seq_count = lax.axis_size("seq")
    seq_bits = seq_count.bit_length() - 1
    upper = lax.axis_index("tok") == 1
    seq_index = lax.axis_index("seq")
    swap = [(0, 1), (1, 0)]
    count = len(pieces) // 2
    half_heads = total.shape[0] // 2
    far = [[] for _ in pieces]
    aggregates = []
    for i in range(count):
        first, size = pieces[i]
        low, rows = first * head_size, size * head_size
        received = lax.ppermute(given[i], "tok", swap)
        if i == 0:
            partner_total = received[rows:]
            partner_total = jnp.concatenate([partner_total[half_heads:], partner_total[:half_heads]])
            decay = jnp.exp(jnp.where(upper, total, partner_total))
        partner = received[:rows]
        own = (apart(own_states) if i else own_states)[low : low + rows]
        factor = spread(decay[first : first + size], head_size)
        far[i].append((received, 0))
        aggregates.append(jnp.where(upper, factor * partner + own, factor * own + partner))
    own_copy = lax.ppermute(own_states, "tok", swap)
    for i in range(count):
        far[count + i].append((own_copy, pieces[i][0] * head_size))
    prefix = jnp.where(upper, partner_total, 0.0)
    gaps = [jnp.where(upper, jnp.zeros_like(total), masked_out)]
    group_decay = jnp.exp(total + partner_total)
    for place in range(seq_bits):
        half = 1 << place
        bases = range(0, seq_count, 2 * half)
        levels = []
        for i in range(count):
            first, size = pieces[i]
            factor = spread(group_decay[first : first + size], head_size)
            first_hop = both_ways(bases, 0) if place == 0 else one_way(bases, half - 1)
            carried = lax.ppermute(aggregates[i], "seq", first_hop)
            for step in range(1, half):
                arrived = lax.ppermute(factor * carried, "seq", one_way(bases, half + step - 1))
                carried = jnp.where(seq_index % (2 * half) == half + step, arrived, carried)
            far[i].append((carried, 0))
            levels.append(carried)
            if place + 1 == seq_bits:
                far[count + i].append((lax.ppermute(carried, "tok", swap), 0))
            aggregates[i] = aggregates[i] + factor * carried
        if place + 1 < seq_bits:
            shared = lax.ppermute(jnp.concatenate(levels), "tok", swap)
            for i in range(count):
                far[count + i].append((shared, pieces[i][0] * head_size))
        gaps.append(jnp.where((seq_index >> place) & 1 == 1, prefix, masked_out))
    return far, gaps


def local(values, key_rows, query_rows, decay_codes, weight_codes, norm_gain):
    heads, tokens = decay_codes.shape
    columns = values.shape[1]
    head_size = columns // heads
    state_size = key_rows.shape[1]
    near_levels = (tokens // BUCKET).bit_length()
    far_count = lax.axis_size("tok").bit_length() + lax.axis_size("seq").bit_length() - 2
    swap = lax.axis_size("tok") == 2
    half = heads // 2
    count = len(PIECE_SHARES)
    sizes = [half * share // sum(PIECE_SHARES) for share in PIECE_SHARES] * 2
    pieces = [(sum(sizes[:i]), size) for i, size in enumerate(sizes)]
    own_rows = [half * head_size] if swap else [n * head_size for _, n in pieces[:count]]

    *given, total, other, source, decay, cum, to_end, keys, queries = pl.pallas_call(
        functools.partial(state_kernel, pieces, swap),
        name="state",
        out_shape=[
            jax.ShapeDtypeStruct((n * head_size + (heads if swap and c == 0 else 0), state_size), f32)
            for c, (_, n) in enumerate(pieces[count:])
        ]
        + [
            jax.ShapeDtypeStruct((heads, LANES), f32),
            jax.ShapeDtypeStruct((columns // 2, tokens), bf16),
            jax.ShapeDtypeStruct((near_levels - 1, heads, tokens), f32),
            jax.ShapeDtypeStruct((near_levels, heads, tokens), f32),
            jax.ShapeDtypeStruct((heads, tokens), f32),
            jax.ShapeDtypeStruct((heads, tokens), f32),
            jax.ShapeDtypeStruct(key_rows.shape, key_rows.dtype),
            jax.ShapeDtypeStruct(query_rows.shape, query_rows.dtype),
        ],
        in_specs=[hbm()] * 4,
        out_specs=[vmem()] * (count + 8),
        scratch_shapes=[
            pltpu.VMEM((tokens, columns // 2), values.dtype),
            pltpu.VMEM(decay_codes.shape, decay_codes.dtype),
            dma((2,)),
            dma((3,)),
        ],
        compiler_params=params,
    )(*(in_hbm(x) for x in (values, key_rows, query_rows, decay_codes)))

    near_call = pl.pallas_call(
        functools.partial(near_kernel, pieces, swap, len(own_rows)),
        name="near",
        out_shape=[pltpu.HBM((n * head_size, tokens), f32) for _, n in pieces]
        + [
            jax.ShapeDtypeStruct((far_count, heads, tokens), f32),
            jax.ShapeDtypeStruct((1, columns), f32),
        ]
        + [jax.ShapeDtypeStruct((n, state_size), f32) for n in own_rows],
        in_specs=[vmem()] * 7 + [hbm()] * 3,
        out_specs=[hbm()] * len(pieces) + [vmem()] * (2 + len(own_rows)),
        scratch_shapes=[
            pltpu.VMEM((tokens // LANES, 2 * LANES, 2 * LANES), bf16),
            pltpu.VMEM((near_levels, heads, tokens), f32),
            pltpu.VMEM(weight_codes.shape, weight_codes.dtype),
            pltpu.VMEM((tokens, columns // 2), values.dtype),
            pltpu.VMEM((columns // 2, tokens), bf16),
            dma((2,)),
            dma((2,)),
            dma(()),
        ]
        + [pltpu.VMEM((n * head_size, tokens), f32) for _, n in pieces]
        + [dma((len(pieces),))],
        compiler_params=params,
    )
    outputs = near_call(
        other,
        queries,
        keys,
        source,
        decay,
        cum,
        to_end,
        in_hbm(weight_codes),
        in_hbm(norm_gain.reshape(1, columns)),
        in_hbm(values),
    )
    near, (far_factor, gain, *own_states) = outputs[: len(pieces)], outputs[len(pieces) :]
    states = [*own_states, *given]

    exchange = exchange_halves if swap else exchange_all
    far, gaps = exchange(states, total, pieces, head_size)
    done = []
    for c, piece in enumerate(pieces):
        rows = piece[1] * head_size
        far_arrays, far_rows = zip(*far[c])
        operands = [near[c], queries, far_factor, gain, *far_arrays, *gaps]
        stores = c + 2 >= len(pieces)
        operands += done if stores else []
        specs = [vmem()] * len(operands)
        aliases = {}
        if c + 1 == len(pieces):
            aliases = {len(operands): 0}
            operands.append(out)
            specs.append(hbm())
        finish_call = pl.pallas_call(
            functools.partial(finish_kernel, pieces[: c + 1], swap, far_count, far_rows, len(done) if stores else 0, stores),
            out_shape=pltpu.HBM((tokens, columns), bf16)
            if stores
            else jax.ShapeDtypeStruct((tokens, rows), bf16),
            in_specs=specs,
            out_specs=hbm() if stores else vmem(),
            scratch_shapes=[pltpu.VMEM((tokens, rows), bf16), dma((len(done) + 1,))] if stores else [],
            input_output_aliases=aliases,
            compiler_params=params,
        )
        out = finish_call(*operands)
        done = [] if stores else [*done, out]
    return out


def solution(mesh):
    return jax.shard_map(
        local,
        mesh=mesh,
        in_specs=(
            P(("parts", "seq", "tok"), "head"),
            P(("parts", "seq", "tok"), None),
            P(("parts", "seq", "tok"), None),
            P("head", ("parts", "seq", "tok")),
            P(None, "head", ("parts", "seq", "tok")),
            P("head"),
        ),
        out_specs=P(("parts", "seq", "tok"), "head"),
        check_vma=False,
    )
```
